128 devices in a mesh: fsdp: 16 (over z, x_lo, core), cols: 8 (over y, x_hi).
Axes of the slice: x: 4 (x_hi: 2, x_lo: 2; x = x_hi * 2 + x_lo), y: 4, z: 4, core: 2. Of those that a mesh axis runs over, the one named last changes fastest.
Arguments:
- weight_query: bfloat16 [5120, 5120], P('fsdp', 'cols'), may hold values from -0.078125 to 0.078125
- low_query: bfloat16 [5120, 32], P('fsdp'), may hold values from -0.078125 to 0.078125
- high_query: bfloat16 [32, 5120], P(None, 'cols'), may hold values from -1 to 1
- weight_key: bfloat16 [5120, 5120], P('fsdp', 'cols'), may hold values from -0.078125 to 0.078125
- low_key: bfloat16 [5120, 32], P('fsdp'), may hold values from -0.078125 to 0.078125
- high_key: bfloat16 [32, 5120], P(None, 'cols'), may hold values from -1 to 1
- weight_value: bfloat16 [5120, 5120], P('fsdp', 'cols'), may hold values from -0.078125 to 0.078125
- low_value: bfloat16 [5120, 32], P('fsdp'), may hold values from -0.078125 to 0.078125
- high_value: bfloat16 [32, 5120], P(None, 'cols'), may hold values from -1 to 1
- weight_mixed: bfloat16 [5120, 5120], P('cols', 'fsdp'), may hold values from -0.078125 to 0.078125
- low_mixed: bfloat16 [5120, 32], P('cols'), may hold values from -0.078125 to 0.078125
- high_mixed: bfloat16 [32, 5120], P(None, 'fsdp'), may hold values from -1 to 1
- norm_train: float32 [5120], P(('fsdp', 'cols')), may hold values from 0.25 to 1.75
- norm_step: float32 [5120], P(('fsdp', 'cols')), may hold values from -0.3 to 0.3
Outputs:
- ready_query: bfloat16 [5120, 5120], P(None, 'cols')
- ready_key: bfloat16 [5120, 5120], P(None, 'cols')
- ready_value: bfloat16 [5120, 5120], P(None, 'cols')
- ready_mixed: bfloat16 [5120, 5120], P('cols')
- serve_norm: bfloat16 [5120], replicated
The draws below stay inside these ranges and needn't reach their ends.
All inputs are finite; a program needn't handle non-finite values.
Results may differ from the reference program's by a relative error of at most 0.001.
Values may be sent and summed in bfloat16 or wider, within the bound.
No kernel may reach another device: no remote copies, remote signals or barrier semaphores. Data moves between devices by JAX's collectives and lax.ppermute only.
A program may use at most 192 MiB of HBM per device.

```python
import jax
import jax.numpy as jnp

D_MODEL = 5120
Q_DIM = 5120
KV_DIM = 5120
RANK = 32


def block_levels(stream_key, extent, pieces, smallest, high):
    level, own = 1.0, jax.random.fold_in(stream_key, 6)
    for dim, shards_of in pieces:
        steps = jnp.exp(jax.random.uniform(jax.random.fold_in(own, dim), (shards_of,), jnp.float32, smallest / len(pieces), high / len(pieces)))
        level = level * jnp.repeat(steps, extent[dim] // shards_of).reshape([-1 if axis == dim else 1 for axis in range(len(extent))])
    return level


def gaussian(stream_key, extent, deviation, limit, split=(), dtype=jnp.bfloat16):
    values = deviation * jax.random.normal(stream_key, extent, jnp.float32)
    if split:
        values = values * block_levels(stream_key, extent, split, -0.22, 0.18)
    return jnp.clip(values, -limit, limit).astype(dtype)


def setup_inputs(seed: int = 0) -> dict:
    arg_keys = jax.random.split(jax.random.key(seed), 15)
    weight_query = gaussian(arg_keys[0], (D_MODEL, Q_DIM), D_MODEL ** -0.5, 0.078125, ((0, 16), (1, 8)))
    low_query = gaussian(arg_keys[1], (D_MODEL, RANK), D_MODEL ** -0.5, 0.078125, ((0, 16),))
    high_query = gaussian(arg_keys[2], (RANK, Q_DIM), RANK ** -0.5, 1.0, ((1, 8),))
    weight_key = gaussian(arg_keys[3], (D_MODEL, KV_DIM), D_MODEL ** -0.5, 0.078125, ((0, 16), (1, 8)))
    low_key = gaussian(arg_keys[4], (D_MODEL, RANK), D_MODEL ** -0.5, 0.078125, ((0, 16),))
    high_key = gaussian(arg_keys[5], (RANK, KV_DIM), RANK ** -0.5, 1.0, ((1, 8),))
    weight_value = gaussian(arg_keys[6], (D_MODEL, KV_DIM), D_MODEL ** -0.5, 0.078125, ((0, 16), (1, 8)))
    low_value = gaussian(arg_keys[7], (D_MODEL, RANK), D_MODEL ** -0.5, 0.078125, ((0, 16),))
    high_value = gaussian(arg_keys[8], (RANK, KV_DIM), RANK ** -0.5, 1.0, ((1, 8),))
    weight_mixed = gaussian(arg_keys[9], (Q_DIM, D_MODEL), Q_DIM ** -0.5, 0.078125, ((0, 8), (1, 16)))
    low_mixed = gaussian(arg_keys[10], (Q_DIM, RANK), Q_DIM ** -0.5, 0.078125, ((0, 8),))
    high_mixed = gaussian(arg_keys[11], (RANK, D_MODEL), RANK ** -0.5, 1.0, ((1, 16),))
    norm_train = jnp.clip(1.0 + 0.15 * jax.random.normal(arg_keys[12], (D_MODEL,), jnp.float32), 0.25, 1.75)
    norm_step = jnp.clip(jax.random.uniform(arg_keys[13], (D_MODEL,), jnp.float32, -0.3, 0.3) * block_levels(arg_keys[13], (D_MODEL,), ((0, 128),), -0.4, 0.0), -0.3, 0.3)
    return dict(weight_query=weight_query, low_query=low_query, high_query=high_query, weight_key=weight_key, low_key=low_key, high_key=high_key, weight_value=weight_value, low_value=low_value, high_value=high_value, weight_mixed=weight_mixed, low_mixed=low_mixed, high_mixed=high_mixed, norm_train=norm_train, norm_step=norm_step)


mix_rate = 2.0


def reference(weight_query, low_query, high_query, weight_key, low_key, high_key, weight_value, low_value, high_value, weight_mixed, low_mixed, high_mixed, norm_train, norm_step):
    latest_query = weight_query.astype(jnp.float32) + mix_rate * jnp.dot(low_query, high_query, preferred_element_type=jnp.float32)
    latest_key = weight_key.astype(jnp.float32) + mix_rate * jnp.dot(low_key, high_key, preferred_element_type=jnp.float32)
    latest_value = weight_value.astype(jnp.float32) + mix_rate * jnp.dot(low_value, high_value, preferred_element_type=jnp.float32)
    latest_mixed = weight_mixed.astype(jnp.float32) + mix_rate * jnp.dot(low_mixed, high_mixed, preferred_element_type=jnp.float32)
    ready_query = latest_query.astype(jnp.bfloat16)
    ready_key = latest_key.astype(jnp.bfloat16)
    ready_value = latest_value.astype(jnp.bfloat16)
    ready_mixed = latest_mixed.astype(jnp.bfloat16)
    serve_norm = (norm_train + norm_step).astype(jnp.bfloat16)
    return ready_query, ready_key, ready_value, ready_mixed, serve_norm
```

```python
import jax
import jax.numpy as jnp
from jax import lax
from jax.experimental import pallas as pl
from jax.experimental.pallas import tpu as pltpu
from jax.sharding import PartitionSpec as P


mix_rate = 2.0
BLOCK = 320
WIDTH = 640
HEAD = 256
ZS = 4

Z_UP = [(f, (f + 4) % 16) for f in range(16)]
Z_DOWN = [(f, (f - 4) % 16) for f in range(16)]
X_SWAP = [(f, f ^ 2) for f in range(16)]
CORE_SWAP = [(f, f ^ 1) for f in range(16)]
HI_SWAP = [(k, k ^ 1) for k in range(8)]


def y_up(s):
    return [(k, (k + 2 * s) % 8) for k in range(8)]


def send(a, perm, axis="fsdp"):
    return lax.ppermute(a, axis, perm)


def updated(weight, low, high):
    product = jnp.dot(low, high, preferred_element_type=jnp.float32)
    return (weight.astype(jnp.float32) + mix_rate * product).astype(jnp.bfloat16)


def copies_of(kind, ref, outs, dz, dx, dc, place):
    z, x, c = place
    chip = lax.rem(z - dz + ZS, ZS) * 2 + (x + dx - 2 * x * dx)
    core = c + dc - 2 * c * dc
    row = pl.multiple_of(chip * (2 * BLOCK) + core * BLOCK, 64)
    ready_query, ready_key, ready_value, ready_mixed = outs
    if kind == "b1":
        return [(ref, ready_query.at[pl.ds(row, BLOCK), :])]
    if kind == "b2":
        return [(ref, ready_key.at[pl.ds(row, HEAD), :])]
    if kind == "a1":
        return [(ref, ready_value.at[pl.ds(row, BLOCK), :])]
    upper = pl.multiple_of(core * BLOCK, 64)
    left = pl.multiple_of(chip * WIDTH, 128)
    tail = pl.multiple_of(row + HEAD, 64)
    return [
        (ref.at[pl.ds(0, BLOCK), :], ready_mixed.at[pl.ds(upper, BLOCK), pl.ds(left, WIDTH)]),
        (ref.at[pl.ds(BLOCK, BLOCK - HEAD), :], ready_key.at[pl.ds(tail, BLOCK - HEAD), :]),
    ]


def assemble(place, pieces, outs):
    n = len(pieces)
    n_copies = sum(2 if p[0] == "a2" else 1 for p in pieces)

    def body(place_ref, *refs):
        sems = refs[-1]
        out_refs = refs[-5:-1]
        where = (place_ref[0], place_ref[1], place_ref[2])
        todo = []
        for (kind, dz, dx, dc, _), ref in zip(pieces, refs[:n]):
            todo += copies_of(kind, ref, out_refs, dz, dx, dc, where)
        started = [pltpu.make_async_copy(s, t, sems.at[i]) for i, (s, t) in enumerate(todo)]
        for copy in started:
            copy.start()
        for copy in started:
            copy.wait()

    shapes = [jax.ShapeDtypeStruct((16 * BLOCK, WIDTH), jnp.bfloat16)] * 3
    shapes.append(jax.ShapeDtypeStruct((WIDTH, 16 * BLOCK), jnp.bfloat16))
    before = [] if outs is None else list(outs)
    any_spec = pl.BlockSpec(memory_space=pl.ANY)
    return pl.pallas_call(
        body,
        out_shape=shapes,
        in_specs=[pl.BlockSpec(memory_space=pltpu.SMEM)] + [any_spec] * (n + len(before)),
        out_specs=[any_spec] * 4,
        scratch_shapes=[pltpu.SemaphoreType.DMA((n_copies,))],
        input_output_aliases={1 + n + i: i for i in range(len(before))},
        compiler_params=pltpu.CompilerParams(vmem_limit_bytes=1 << 20),
    )(place, *[p[-1] for p in pieces], *before)


def gathered_norm(norm_train, norm_step, z, x, c):
    mine = (norm_train + norm_step).astype(jnp.bfloat16)
    rows = jnp.pad(mine, (0, 88))[None, :]
    rows = jnp.concatenate([rows] + [send(rows, y_up(s), "cols") for s in (1, 2, 3)], 0)
    rows = jnp.concatenate([rows, send(rows, HI_SWAP, "cols")], 0)
    rows = jnp.concatenate([rows, send(rows, CORE_SWAP)], 0)
    rows = jnp.concatenate([rows, send(rows, X_SWAP)], 0)
    below = send(rows, Z_UP)
    rows = jnp.concatenate([rows, below, send(below, Z_UP), send(rows, Z_DOWN)], 0)
    k = lax.axis_index("cols")
    y, hi = k // 2, k % 2
    r = lax.iota(jnp.int32, 128)
    col = ((y - r % 4) % 4) * 2 + (hi ^ (r // 4 % 2))
    part = ((z - r // 32) % 4) * 4 + (x ^ (r // 16 % 2)) * 2 + (c ^ (r // 8 % 2))
    place = (lax.iota(jnp.int32, 128)[:, None] == (part * 8 + col)[None, :]).astype(jnp.bfloat16)
    ordered = jnp.dot(place, rows, preferred_element_type=jnp.float32).astype(jnp.bfloat16)
    return ordered[:, :40].reshape(5120)


def per_device(
    weight_query, low_query, high_query,
    weight_key, low_key, high_key,
    weight_value, low_value, high_value,
    weight_mixed, low_mixed, high_mixed,
    norm_train, norm_step,
):
    f = lax.axis_index("fsdp")
    z, x, c = f // 4, f // 2 % 2, f % 2
    place = jnp.stack([z, x, c]).astype(jnp.int32)

    b1 = updated(weight_query, low_query, high_query)
    b2 = updated(weight_key[:HEAD], low_key[:HEAD], high_key)
    key_tail = updated(weight_key[HEAD:], low_key[HEAD:], high_key)
    a1 = updated(weight_value, low_value, high_value)
    mixed = updated(weight_mixed, low_mixed, high_mixed)
    keep = lax.dynamic_slice(mixed, (c * BLOCK, 0), (BLOCK, BLOCK))
    give = lax.dynamic_slice(mixed, ((1 - c) * BLOCK, 0), (BLOCK, BLOCK))
    got = send(give, CORE_SWAP)
    left = jnp.where(c == 0, keep, got)
    right = jnp.where(c == 0, got, keep)
    a2 = jnp.concatenate([jnp.concatenate([left, right], 1), key_tail], 0)

    have = {}
    for kind, own in (("b1", b1), ("b2", b2), ("a1", a1), ("a2", a2)):
        have[kind, 0, 0] = own
        have[kind, 1, 0] = send(own, Z_UP)
        have[kind, 3, 0] = send(own, Z_DOWN)
        have[kind, 0, 1] = send(own, X_SWAP)
    have["b1", 2, 0] = send(have["b1", 1, 0], Z_UP)
    have["b2", 2, 0] = send(have["b2", 3, 0], Z_DOWN)
    for kind in ("a1", "a2"):
        have[kind, 1, 1] = send(have[kind, 0, 1], Z_UP)
        have[kind, 3, 1] = send(have[kind, 0, 1], Z_DOWN)
    have["a1", 2, 0] = send(have["a1", 1, 0], Z_UP)
    have["a2", 2, 0] = send(have["a2", 3, 0], Z_DOWN)
    have["a1", 2, 1] = send(have["a1", 1, 1], Z_UP)
    have["a2", 2, 1] = send(have["a2", 3, 1], Z_DOWN)
    for dz in (1, 3, 2):
        for kind in ("b1", "b2"):
            have[kind, dz, 1] = send(have[kind, dz, 0], X_SWAP)

    serve_norm = gathered_norm(norm_train, norm_step, z, x, c)

    def both(keys):
        out = []
        for kind, dz, dx in keys:
            piece = have[kind, dz, dx]
            out.append((kind, dz, dx, 0, piece))
            out.append((kind, dz, dx, 1, send(piece, CORE_SWAP)))
        return out

    kinds = ("b1", "b2", "a1", "a2")
    first = [(k, dz, dx) for dz, dx in ((0, 0), (1, 0), (3, 0), (0, 1)) for k in kinds]
    second = [(k, dz, dx) for dz, dx in ((2, 0), (1, 1), (3, 1)) for k in kinds]
    last = [(k, 2, 1) for k in kinds]
    outs = None
    for keys in (first, second, last):
        outs = assemble(place, both(keys), outs)
    return (*outs, serve_norm)


def solution(mesh):
    in_specs = (
        P("fsdp", "cols"), P("fsdp", None), P(None, "cols"),
        P("fsdp", "cols"), P("fsdp", None), P(None, "cols"),
        P("fsdp", "cols"), P("fsdp", None), P(None, "cols"),
        P("cols", "fsdp"), P("cols", None), P(None, "fsdp"),
        P(("fsdp", "cols")), P(("fsdp", "cols")),
    )
    out_specs = (P(None, "cols"), P(None, "cols"), P(None, "cols"), P("cols", None), P())
    return jax.shard_map(
        per_device, mesh=mesh, in_specs=in_specs, out_specs=out_specs, check_vma=False
    )
```

```python
import jax
import jax.numpy as jnp
from jax import lax
from jax.experimental import pallas as pl
from jax.experimental.pallas import tpu as pltpu
from jax.sharding import PartitionSpec as P


mix_rate = 2.0
BLOCK = 320
WIDTH = 640
HEAD = 256
B_ROWS = BLOCK + HEAD
A_ROWS = 3 * BLOCK - HEAD

Z_UP = [(f, (f + 4) % 16) for f in range(16)]
Z_DOWN = [(f, (f - 4) % 16) for f in range(16)]
X_SWAP = [(f, f ^ 2) for f in range(16)]
CORE_SWAP = [(f, f ^ 1) for f in range(16)]
HI_SWAP = [(k, k ^ 1) for k in range(8)]


def y_up(s):
    return [(k, (k + 2 * s) % 8) for k in range(8)]


def send(a, perm, axis="fsdp"):
    return lax.ppermute(a, axis, perm)


def updated(weight, low, high):
    product = jnp.dot(low, high, preferred_element_type=jnp.float32)
    return (weight.astype(jnp.float32) + mix_rate * product).astype(jnp.bfloat16)


PARTS = {
    "b": ((0, BLOCK, 0, 0), (BLOCK, B_ROWS, 1, 0)),
    "a": ((0, BLOCK, 2, 0), (BLOCK, 2 * BLOCK, 3, 0), (2 * BLOCK, A_ROWS, 1, HEAD)),
}


def rows_of(piece):
    return piece[2] - piece[1]


def copies_of(piece, ref, base, outs, dc, place):
    kind, low, high, dz, dx = piece
    z, x, c = place
    chip = lax.rem(z - dz + 4, 4) * 2 + (x + dx - 2 * x * dx)
    core = c + dc - 2 * c * dc
    found = []
    for first, end, which, row in PARTS[kind]:
        lo, hi = max(first, low), min(end, high)
        if lo >= hi:
            continue
        n, row = hi - lo, row + lo - first
        source = ref.at[pl.ds(base + lo - low, n), :]
        if which == 3:
            at = (pl.ds(pl.multiple_of(core * BLOCK + row, 16), n), pl.ds(pl.multiple_of(chip * WIDTH, 128), WIDTH))
        else:
            at = (pl.ds(pl.multiple_of(chip * (2 * BLOCK) + core * BLOCK + row, 16), n), slice(None))
        found.append((source, outs[which].at[at]))
    return found


def assemble(place, own, other, outs, stack=True):
    n_own, n_other = len(own), len(other)
    rows = sum(rows_of(p) for p, _ in own)
    before = [] if outs is None else list(outs)

    def body(place_ref, *refs):
        own_refs, other_refs = refs[:n_own], refs[n_own : n_own + n_other]
        refs = refs[n_own + n_other + len(before) :]
        out_refs, refs = refs[:4], refs[4:]
        stack_ref, load_sem, store_sem = refs if own else (None, None, refs[0])
        where = (place_ref[0], place_ref[1], place_ref[2])
        loads, base = [], 0
        for i, ((piece, _), ref) in enumerate(zip(own, own_refs)):
            n = rows_of(piece)
            loads.append(pltpu.make_async_copy(ref, stack_ref.at[pl.ds(base, n), :], load_sem.at[i]))
            loads[-1].start()
            base += n
        stores = []

        def put(piece, ref, base, dc):
            for source, target in copies_of(piece, ref, base, out_refs, dc, where):
                stores.append(pltpu.make_async_copy(source, target, store_sem.at[len(stores)]))
                stores[-1].start()

        for (pieces, _), ref in zip(other, other_refs):
            base = 0
            for piece in pieces:
                put(piece, ref, base, 1)
                base += rows_of(piece)
        base = 0
        for load, (piece, _) in zip(loads, own):
            load.wait()
            put(piece, stack_ref, base, 0)
            base += rows_of(piece)
        for store in stores:
            store.wait()

    shapes = [jax.ShapeDtypeStruct((16 * BLOCK, WIDTH), jnp.bfloat16)] * 3
    shapes.append(jax.ShapeDtypeStruct((WIDTH, 16 * BLOCK), jnp.bfloat16))
    any_spec = pl.BlockSpec(memory_space=pl.ANY)
    vmem_spec = pl.BlockSpec(memory_space=pltpu.VMEM)
    out_specs = [any_spec] * 4
    scratch = []
    if own and stack:
        shapes.append(jax.ShapeDtypeStruct((rows, WIDTH), jnp.bfloat16))
        out_specs.append(vmem_spec)
    elif own:
        scratch.append(pltpu.VMEM((rows, WIDTH), jnp.bfloat16))
    if own:
        scratch.append(pltpu.SemaphoreType.DMA((n_own,)))
    pieces = [p for p, _ in own] + [p for many, _ in other for p in many]
    scratch.append(pltpu.SemaphoreType.DMA((3 * len(pieces),)))
    call = pl.pallas_call(
        body,
        out_shape=shapes,
        in_specs=[pl.BlockSpec(memory_space=pltpu.SMEM)] + [any_spec] * n_own + [vmem_spec] * n_other + [any_spec] * len(before),
        out_specs=out_specs,
        scratch_shapes=scratch,
        input_output_aliases={1 + n_own + n_other + i: i for i in range(len(before))},
        compiler_params=pltpu.CompilerParams(vmem_limit_bytes=12 << 20),
    )
    result = call(place, *[v for _, v in own], *[v for _, v in other], *before)
    return result[:4], (result[4] if own and stack else None)


def gathered_norm(norm_train, norm_step, z, x, c):
    mine = (norm_train + norm_step).astype(jnp.bfloat16)
    rows = jnp.pad(mine, (0, 88))[None, :]
    rows = jnp.concatenate([rows] + [send(rows, y_up(s), "cols") for s in (1, 2, 3)], 0)
    rows = jnp.concatenate([rows, send(rows, HI_SWAP, "cols")], 0)
    rows = jnp.concatenate([rows, send(rows, CORE_SWAP)], 0)
    rows = jnp.concatenate([rows, send(rows, X_SWAP)], 0)
    below = send(rows, Z_UP)
    rows = jnp.concatenate([rows, below, send(below, Z_UP), send(rows, Z_DOWN)], 0)
    k = lax.axis_index("cols")
    y, hi = k // 2, k % 2
    r = lax.iota(jnp.int32, 128)
    col = ((y - r % 4) % 4) * 2 + (hi ^ (r // 4 % 2))
    part = ((z - r // 32) % 4) * 4 + (x ^ (r // 16 % 2)) * 2 + (c ^ (r // 8 % 2))
    place = (lax.iota(jnp.int32, 128)[:, None] == (part * 8 + col)[None, :]).astype(jnp.bfloat16)
    ordered = jnp.dot(place, rows, preferred_element_type=jnp.float32).astype(jnp.bfloat16)
    return ordered[:, :40].reshape(5120)


def per_device(
    weight_query, low_query, high_query,
    weight_key, low_key, high_key,
    weight_value, low_value, high_value,
    weight_mixed, low_mixed, high_mixed,
    norm_train, norm_step,
):
    f = lax.axis_index("fsdp")
    z, x, c = f // 4, f // 2 % 2, f % 2
    place = jnp.stack([z, x, c]).astype(jnp.int32)

    b = jnp.concatenate(
        [
            updated(weight_query, low_query, high_query),
            updated(weight_key[:HEAD], low_key[:HEAD], high_key),
        ],
        0,
    )
    mixed = updated(weight_mixed, low_mixed, high_mixed)
    keep = lax.dynamic_slice(mixed, (c * BLOCK, 0), (BLOCK, BLOCK))
    give = lax.dynamic_slice(mixed, ((1 - c) * BLOCK, 0), (BLOCK, BLOCK))
    got = send(give, CORE_SWAP)
    left = jnp.where(c == 0, keep, got)
    right = jnp.where(c == 0, got, keep)
    a = jnp.concatenate(
        [
            updated(weight_value, low_value, high_value),
            jnp.concatenate([left, right], 1),
            updated(weight_key[HEAD:], low_key[HEAD:], high_key),
        ],
        0,
    )

    hb, ha = B_ROWS // 2, A_ROWS // 2
    b_up, b_down, b_x = send(b, Z_UP), send(b, Z_DOWN), send(b, X_SWAP)
    a_up, a_down, a_x = send(a, Z_UP), send(a, Z_DOWN), send(a, X_SWAP)
    b_up2, b_down2 = send(b_up[:hb], Z_UP), send(b_down[hb:], Z_DOWN)
    bx_up, bx_down = send(b_up, X_SWAP), send(b_down, X_SWAP)
    ax_up, ax_down = send(a_x, Z_UP), send(a_x, Z_DOWN)
    a_up2, a_down2 = send(a_up[:ha], Z_UP), send(a_down[ha:], Z_DOWN)
    bx_up2, bx_down2 = send(b_up2, X_SWAP), send(b_down2, X_SWAP)
    ax_up2, ax_down2 = send(ax_up[:ha], Z_UP), send(ax_down[ha:], Z_DOWN)

    serve_norm = gathered_norm(norm_train, norm_step, z, x, c)

    def whole(kind, dz, dx, v):
        return ((kind, 0, B_ROWS if kind == "b" else A_ROWS, dz, dx), v)

    def top(kind, dx, v):
        return ((kind, 0, hb if kind == "b" else ha, 2, dx), v)

    def bottom(kind, dx, v):
        return ((kind, hb, B_ROWS, 2, dx) if kind == "b" else (kind, ha, A_ROWS, 2, dx), v)

    def swapped(own, stack):
        return ([p for p, _ in own], send(stack, CORE_SWAP))

    own1 = [whole("b", 0, 0, b), whole("a", 0, 0, a), whole("b", 1, 0, b_up), whole("b", 3, 0, b_down), whole("b", 0, 1, b_x)]
    outs, stack1 = assemble(place, own1, [], None)
    own2 = [whole("a", 1, 0, a_up), whole("a", 3, 0, a_down), whole("a", 0, 1, a_x), top("b", 0, b_up2), bottom("b", 0, b_down2)]
    outs, stack2 = assemble(place, own2, [swapped(own1, stack1)], outs)
    own3 = [whole("a", 1, 1, ax_up), whole("a", 3, 1, ax_down), whole("b", 1, 1, bx_up), whole("b", 3, 1, bx_down), top("a", 0, a_up2), bottom("a", 0, a_down2)]
    outs, stack3 = assemble(place, own3, [swapped(own2, stack2)], outs)
    own4 = [top("a", 1, ax_up2), bottom("a", 1, ax_down2), top("b", 1, bx_up2), bottom("b", 1, bx_down2)]
    late = [([p], send(v, CORE_SWAP)) for p, v in own4]
    outs, _ = assemble(place, own4, [swapped(own3, stack3)], outs, stack=False)
    outs, _ = assemble(place, [], late, outs)
    return (*outs, serve_norm)


def solution(mesh):
    in_specs = (
        P("fsdp", "cols"), P("fsdp", None), P(None, "cols"),
        P("fsdp", "cols"), P("fsdp", None), P(None, "cols"),
        P("fsdp", "cols"), P("fsdp", None), P(None, "cols"),
        P("cols", "fsdp"), P("cols", None), P(None, "fsdp"),
        P(("fsdp", "cols")), P(("fsdp", "cols")),
    )
    out_specs = (P(None, "cols"), P(None, "cols"), P(None, "cols"), P("cols", None), P())

    return jax.shard_map(per_device, mesh=mesh, in_specs=in_specs, out_specs=out_specs, check_vma=False)
```

```python
import jax
import jax.numpy as jnp
from jax import lax
from jax.experimental import pallas as pl
from jax.experimental.pallas import tpu as pltpu
from jax.sharding import PartitionSpec as P


mix_rate = 2.0
BLOCK = 320
WIDTH = 640
HEAD = 256
B_ROWS = BLOCK + HEAD
A_ROWS = 3 * BLOCK - HEAD

X_SWAP = [(f, f ^ 2) for f in range(16)]
CORE_SWAP = [(f, f ^ 1) for f in range(16)]
HI_SWAP = [(k, k ^ 1) for k in range(8)]


def y_by(s):
    return [(k, (k + 2 * s) % 8) for k in range(8)]


def z_by(s):
    return [(f, (f + 4 * s) % 16) for f in range(16)]


def send(a, perm, axis="fsdp"):
    return lax.ppermute(a, axis, perm)


def updated(weight, low, high):
    product = jnp.dot(low, high, preferred_element_type=jnp.float32)
    return (weight.astype(jnp.float32) + mix_rate * product).astype(jnp.bfloat16)


PARTS = {
    "b": ((0, BLOCK, 0, 0), (BLOCK, B_ROWS, 1, 0)),
    "a": ((0, BLOCK, 2, 0), (BLOCK, 2 * BLOCK, 3, 0), (2 * BLOCK, A_ROWS, 1, HEAD)),
}


def rows_of(piece):
    return piece[2] - piece[1]


def copies_of(piece, ref, base, outs, dc, place):
    kind, low, high, dz, dx = piece
    z, x, c = place
    chip = lax.rem(z - dz + 4, 4) * 2 + (x + dx - 2 * x * dx)
    core = c + dc - 2 * c * dc
    found = []
    for first, end, which, row in PARTS[kind]:
        lo, hi = max(first, low), min(end, high)
        if lo >= hi:
            continue
        n, row = hi - lo, row + lo - first
        source = ref.at[pl.ds(base + lo - low, n), :]
        if which == 3:
            at = (pl.ds(pl.multiple_of(core * BLOCK + row, 16), n), pl.ds(pl.multiple_of(chip * WIDTH, 128), WIDTH))
        else:
            at = (pl.ds(pl.multiple_of(chip * (2 * BLOCK) + core * BLOCK + row, 16), n), slice(None))
        found.append((source, outs[which].at[at]))
    return found


def assemble(place, own, other, outs, stack=True, extra=None):
    n_own, n_other = len(own), len(other)
    rows = sum(rows_of(p) for p, _ in own)
    before = [] if outs is None else list(outs)
    extras = [] if extra is None else [extra]

    def body(place_ref, *refs):
        own_refs, other_refs = refs[:n_own], refs[n_own : n_own + n_other]
        refs = refs[n_own + n_other + len(before) + len(extras) :]
        out_refs, refs = refs[:4], refs[4:]
        stack_ref, load_sem, store_sem = refs if own else (None, None, refs[0])
        where = (place_ref[0], place_ref[1], place_ref[2])
        loads, base = [], 0
        for i, ((piece, _), ref) in enumerate(zip(own, own_refs)):
            n = rows_of(piece)
            loads.append(pltpu.make_async_copy(ref, stack_ref.at[pl.ds(base, n), :], load_sem.at[i]))
            loads[-1].start()
            base += n
        stores = []

        def put(piece, ref, base, dc):
            for source, target in copies_of(piece, ref, base, out_refs, dc, where):
                stores.append(pltpu.make_async_copy(source, target, store_sem.at[len(stores)]))
                stores[-1].start()

        for (pieces, _), ref in zip(other, other_refs):
            base = 0
            for piece in pieces:
                put(piece, ref, base, 1)
                base += rows_of(piece)
        base = 0
        for load, (piece, _) in zip(loads, own):
            load.wait()
            put(piece, stack_ref, base, 0)
            base += rows_of(piece)
        for store in stores:
            store.wait()

    shapes = [jax.ShapeDtypeStruct((16 * BLOCK, WIDTH), jnp.bfloat16)] * 3
    shapes.append(jax.ShapeDtypeStruct((WIDTH, 16 * BLOCK), jnp.bfloat16))
    any_spec = pl.BlockSpec(memory_space=pl.ANY)
    vmem_spec = pl.BlockSpec(memory_space=pltpu.VMEM)
    out_specs = [any_spec] * 4
    scratch = []
    if own and stack:
        shapes.append(jax.ShapeDtypeStruct((rows, WIDTH), jnp.bfloat16))
        out_specs.append(vmem_spec)
    elif own:
        scratch.append(pltpu.VMEM((rows, WIDTH), jnp.bfloat16))
    if own:
        scratch.append(pltpu.SemaphoreType.DMA((n_own,)))
    pieces = [p for p, _ in own] + [p for many, _ in other for p in many]
    scratch.append(pltpu.SemaphoreType.DMA((3 * len(pieces),)))
    call = pl.pallas_call(
        body,
        out_shape=shapes,
        in_specs=[pl.BlockSpec(memory_space=pltpu.SMEM)] + [any_spec] * n_own + [vmem_spec] * n_other + [any_spec] * (len(before) + len(extras)),
        out_specs=out_specs,
        scratch_shapes=scratch,
        input_output_aliases={1 + n_own + n_other + i: i for i in range(len(before))},
        compiler_params=pltpu.CompilerParams(vmem_limit_bytes=12 << 20),
    )
    result = call(place, *[v for _, v in own], *[v for _, v in other], *before, *extras)
    return result[:4], (result[4] if own and stack else None)


def gathered_norm(norm_train, norm_step, z, x, c):
    mine = (norm_train + norm_step).astype(jnp.bfloat16)
    rows = jnp.pad(mine, (0, 88))[None, :]
    rows = jnp.concatenate([rows, send(rows, CORE_SWAP)], 0)
    across = send(rows, X_SWAP)
    rows = jnp.concatenate([rows, across], 0)
    others = [send(rows, z_by(s)) for s in (1, 2, 3)]
    rows = jnp.concatenate([rows] + others, 0)
    rows = jnp.concatenate([rows] + [send(rows, y_by(s), "cols") for s in (1, 2, 3)], 0)
    rows = jnp.concatenate([rows, send(rows, HI_SWAP, "cols")], 0)
    k = lax.axis_index("cols")
    y, hi = k // 2, k % 2
    r = lax.iota(jnp.int32, 128)
    part = ((z - r // 4 % 4) % 4) * 4 + (x ^ (r // 2 % 2)) * 2 + (c ^ (r % 2))
    col = ((y - r // 16 % 4) % 4) * 2 + (hi ^ (r // 64))
    place = (lax.iota(jnp.int32, 128)[:, None] == (part * 8 + col)[None, :]).astype(jnp.bfloat16)
    ordered = jnp.dot(place, rows, preferred_element_type=jnp.float32).astype(jnp.bfloat16)
    return ordered[:, :40].reshape(5120)


def per_device(
    weight_query, low_query, high_query,
    weight_key, low_key, high_key,
    weight_value, low_value, high_value,
    weight_mixed, low_mixed, high_mixed,
    norm_train, norm_step,
):
    f = lax.axis_index("fsdp")
    z, x, c = f // 4, f // 2 % 2, f % 2
    place = jnp.stack([z, x, c]).astype(jnp.int32)

    b = jnp.concatenate(
        [
            updated(weight_query, low_query, high_query),
            updated(weight_key[:HEAD], low_key[:HEAD], high_key),
        ],
        0,
    )
    mixed = updated(weight_mixed, low_mixed, high_mixed)
    keep = lax.dynamic_slice(mixed, (c * BLOCK, 0), (BLOCK, BLOCK))
    give = lax.dynamic_slice(mixed, ((1 - c) * BLOCK, 0), (BLOCK, BLOCK))
    got = send(give, CORE_SWAP)
    left = jnp.where(c == 0, keep, got)
    right = jnp.where(c == 0, got, keep)
    a = jnp.concatenate(
        [
            updated(weight_value, low_value, high_value),
            jnp.concatenate([left, right], 1),
            updated(weight_key[HEAD:], low_key[HEAD:], high_key),
        ],
        0,
    )

    hb, ha = B_ROWS // 2, A_ROWS // 2
    b_up, b_down, b_x = send(b, z_by(1)), send(b, z_by(3)), send(b, X_SWAP)
    a_up, a_down, a_x = send(a, z_by(1)), send(a, z_by(3)), send(a, X_SWAP)
    b_up2, b_down2 = send(b_up[:hb], z_by(1)), send(b_down[hb:], z_by(3))
    bx_up, bx_down = send(b_up, X_SWAP), send(b_down, X_SWAP)
    ax_up, ax_down = send(a_x, z_by(1)), send(a_x, z_by(3))
    a_up2, a_down2 = send(a_up[:ha], z_by(1)), send(a_down[ha:], z_by(3))
    bx_up2, bx_down2 = send(b_up2, X_SWAP), send(b_down2, X_SWAP)
    ax_up2, ax_down2 = send(ax_up[:ha], z_by(1)), send(ax_down[ha:], z_by(3))

    serve_norm = gathered_norm(norm_train, norm_step, z, x, c)

    def whole(kind, dz, dx, v):
        return ((kind, 0, B_ROWS if kind == "b" else A_ROWS, dz, dx), v)

    def top(kind, dx, v):
        return ((kind, 0, hb if kind == "b" else ha, 2, dx), v)

    def bottom(kind, dx, v):
        return ((kind, hb, B_ROWS, 2, dx) if kind == "b" else (kind, ha, A_ROWS, 2, dx), v)

    def swapped(own, stack):
        return ([p for p, _ in own], send(stack, CORE_SWAP))

    own1 = [whole("b", 0, 0, b), whole("a", 0, 0, a), whole("b", 1, 0, b_up), whole("b", 3, 0, b_down), whole("b", 0, 1, b_x)]
    outs, stack1 = assemble(place, own1, [], None)
    own2 = [whole("a", 1, 0, a_up), whole("a", 3, 0, a_down), whole("a", 0, 1, a_x), top("b", 0, b_up2), bottom("b", 0, b_down2)]
    outs, stack2 = assemble(place, own2, [swapped(own1, stack1)], outs)
    own3 = [whole("a", 1, 1, ax_up), whole("a", 3, 1, ax_down), whole("b", 1, 1, bx_up)]
    outs, stack3 = assemble(place, own3, [swapped(own2, stack2)], outs)
    own4 = [whole("b", 3, 1, bx_down), top("a", 0, a_up2), bottom("a", 0, a_down2)]
    late = [([p], send(v, CORE_SWAP)) for p, v in own4]
    outs, _ = assemble(place, own4, [swapped(own3, stack3)], outs, stack=False, extra=serve_norm)
    own5 = [top("b", 1, bx_up2), bottom("b", 1, bx_down2), top("a", 1, ax_up2), bottom("a", 1, ax_down2)]
    last = [([p], send(v, CORE_SWAP)) for p, v in own5]
    outs, _ = assemble(place, own5, late, outs, stack=False)
    outs, _ = assemble(place, [], last, outs)
    return (*outs, serve_norm)


def solution(mesh):
    in_specs = (
        P("fsdp", "cols"), P("fsdp", None), P(None, "cols"),
        P("fsdp", "cols"), P("fsdp", None), P(None, "cols"),
        P("fsdp", "cols"), P("fsdp", None), P(None, "cols"),
        P("cols", "fsdp"), P("cols", None), P(None, "fsdp"),
        P(("fsdp", "cols")), P(("fsdp", "cols")),
    )
    out_specs = (P(None, "cols"), P(None, "cols"), P(None, "cols"), P("cols", None), P())

    return jax.shard_map(per_device, mesh=mesh, in_specs=in_specs, out_specs=out_specs, check_vma=False)
```
